32 devices in a mesh: outer: 4 (over y, core), inner: 8 (over z, x).
Axes of the slice: x: 2, y: 2, z: 4, core: 2. Of those that a mesh axis runs over, the one named last changes fastest.
Arguments:
- queries: bfloat16 [4096, 16, 128], P(('outer', 'inner')), may hold values from -160 to 160
- key_vectors: bfloat16 [4096, 128], P(('outer', 'inner')), may hold values from -6 to 6
- value_vectors: bfloat16 [4096, 128], P(('outer', 'inner')), may hold values from -6 to 6
- doc_lengths: int32 [4], replicated, may hold values from 1 to 1921, 4096 in all
Outputs:
- attended: bfloat16 [4096, 16, 128], P(('outer', 'inner'))
The draws below stay inside these ranges and needn't reach their ends.
All inputs are finite; a program needn't handle non-finite values.
Results may differ from the reference program's by a relative error of at most 0.0037.
Values may be sent and summed in bfloat16 or wider, within the bound.
No kernel may reach another device: no remote copies, remote signals or barrier semaphores. Data moves between devices by JAX's collectives and lax.ppermute only.
A program may use at most 64 MiB of HBM per device.

```python
import math
import jax
import jax.numpy as jnp
import numpy as np
from jax import lax

HEADS = 16
HDIM = 128
TOK_DEV = 128
REACH = 16
TOKENS = 4096
DOCMAX = 1921
DOCS = 4


def paired_draw(key):
    base_keys = jax.random.truncated_normal(jax.random.fold_in(key, 3), -6.0, 6.0, (TOKENS, HDIM), jnp.float32)
    base_queries = jax.random.truncated_normal(jax.random.fold_in(key, 4), -6.0, 6.0, (TOKENS, HEADS, HDIM), jnp.float32)
    return (base_queries, base_keys)


def draw_queries(key, part):
    return paired_draw(key)[0].astype(jnp.bfloat16)


def draw_key_vectors(key, part):
    return paired_draw(key)[1].astype(jnp.bfloat16)


def steps_of(stream_key, dims, pieces, smallest, largest):
    gain, own = 1.0, jax.random.fold_in(stream_key, 6)
    for dim, parts in pieces:
        steps = jnp.exp(jax.random.uniform(jax.random.fold_in(own, dim), (parts,), jnp.float32, smallest / len(pieces), largest / len(pieces)))
        gain = gain * jnp.repeat(steps, dims[dim] // parts).reshape([-1 if axis == dim else 1 for axis in range(len(dims))])
    return gain


def profile(number_of, total, limit, slope):
    portions = [(1 << 20) // math.isqrt(grade ** slope) + 1 for grade in range(2, number_of + 1)]
    surplus, counts = total - limit - (number_of - 1), [1] * (number_of - 1)
    while surplus > 0:
        candidates = [i for i in range(number_of - 1) if counts[i] < limit]
        whole, remaining = sum([portions[i] for i in candidates]), surplus
        for i in candidates:
            extra = min(limit - counts[i], max(1, remaining * portions[i] // whole), surplus)
            counts[i] = counts[i] + extra
            surplus = surplus - extra
    return np.array([limit] + counts)


def uneven(key, count, total, limit, slope):
    if count == 2:
        one = jax.random.randint(key, (), max(1, total - limit), min(limit, total - 1) + 1)
        return jnp.stack([one, total - one])
    sizes = jnp.asarray(profile(count, total, limit, slope), jnp.int32)
    twos = (count - 1) // 2
    giver, receiver = sizes[1:1 + 2 * twos:2], sizes[2:2 + 2 * twos:2]
    room = jnp.minimum(giver - 1, limit - receiver)
    moved = jax.random.randint(jax.random.fold_in(key, 1), (twos,), 0, 1 << 20) % (room + 1)
    sizes = sizes.at[1:1 + 2 * twos:2].set(giver - moved).at[2:2 + 2 * twos:2].set(receiver + moved)
    return sizes[jax.random.permutation(jax.random.fold_in(key, 2), count)]


def bell_draw(own_key, dims, scale, limit, split=(), held_as=jnp.bfloat16):
    factor_of = steps_of(own_key, dims, split, -0.22, 0.18) if split else 1.0
    values = jax.random.normal(own_key, dims, jnp.float32) * scale * factor_of
    return jnp.minimum(jnp.maximum(values, -limit), limit).astype(held_as)


def setup_inputs(seed: int = 0) -> dict:
    key_list = jax.random.split(jax.random.key(seed), 5)
    return {
        "queries": draw_queries(jax.random.fold_in(key_list[4], 71), 0),
        "key_vectors": draw_key_vectors(jax.random.fold_in(key_list[4], 71), 0),
        "value_vectors": bell_draw(key_list[2], (TOKENS, HDIM), 1.0, 6.0, ((0, 32),)),
        "doc_lengths": uneven(key_list[3], DOCS, TOKENS, DOCMAX, 2).astype(jnp.int32),
    }


def segment_ids(positions, starts):
    inside = (starts[None, :] <= positions[:, None]).astype(jnp.int32)
    return jnp.sum(inside, axis=1).astype(jnp.int32) - 1


def update(running, query_rows, key_rows, value_rows, query_seg, query_pos, key_seg, key_pos):
    row_max, row_sum, accumulated = running
    scale_factor = query_rows.shape[-1] ** -0.5
    scores = jnp.einsum("thd,kd->thk", query_rows.astype(jnp.float32), key_rows.astype(jnp.float32)) * scale_factor
    allowed = (query_seg[:, None] == key_seg[None, :]) & (key_pos[None, :] <= query_pos[:, None])
    scores = jnp.where(allowed[:, None, :], scores, -1e30)
    new_max = jnp.maximum(row_max, jnp.max(scores, axis=-1))
    rescale = jnp.exp(row_max - new_max)
    weights = jnp.exp(scores - new_max[..., None])
    row_sum = rescale * row_sum + jnp.sum(weights, axis=-1)
    rounded = weights.astype(jnp.bfloat16)
    product = jnp.einsum("thk,kd->thd", rounded.astype(jnp.float32), value_rows.astype(jnp.float32))
    accumulated = rescale[..., None] * accumulated + product
    return (new_max, row_sum, accumulated)


def reference(queries, key_vectors, value_vectors, doc_lengths):
    starts = (jnp.cumsum(doc_lengths) - doc_lengths).astype(jnp.int32)
    blocks = TOKENS // TOK_DEV
    padding = jnp.zeros(((REACH - 1) * TOK_DEV, HDIM), key_vectors.dtype)
    key_padded = jnp.concatenate([padding, key_vectors], axis=0)
    value_padded = jnp.concatenate([padding, value_vectors], axis=0)
    offsets = jnp.arange(TOK_DEV, dtype=jnp.int32)

    def query_block(block):
        query_rows = lax.dynamic_slice_in_dim(queries, (block * TOK_DEV).astype(jnp.int32), TOK_DEV, 0)
        query_pos = block * TOK_DEV + offsets
        query_seg = segment_ids(query_pos, starts)
        running = (jnp.full((TOK_DEV, HEADS), -1e30, jnp.float32),
                   jnp.zeros((TOK_DEV, HEADS), jnp.float32),
                   jnp.zeros((TOK_DEV, HEADS, HDIM), jnp.float32))
        for distance in range(REACH - 1, -1, -1):
            begin = ((block - distance + REACH - 1) * TOK_DEV).astype(jnp.int32)
            key_rows = lax.dynamic_slice_in_dim(key_padded, begin, TOK_DEV, 0)
            value_rows = lax.dynamic_slice_in_dim(value_padded, begin, TOK_DEV, 0)
            key_pos = (block - distance) * TOK_DEV + offsets
            key_seg = segment_ids(key_pos, starts)
            running = update(running, query_rows, key_rows, value_rows, query_seg, query_pos, key_seg, key_pos)
        return (running[2] / running[1][..., None]).astype(jnp.bfloat16)

    result = lax.map(query_block, jnp.arange(blocks, dtype=jnp.int32))
    return result.reshape(TOKENS, HEADS, HDIM)
```

```python
import functools
import math

import jax
import jax.numpy as jnp
from jax import lax
from jax.experimental import pallas as pl
from jax.experimental.pallas import tpu as pltpu
from jax.sharding import PartitionSpec as P

REACH = 16
AXES = ("outer", "inner")
NEG = -1e30


def rotate(x, count, by):
    return lax.ppermute(x, AXES, [(i, (i + by) % count) for i in range(count)])


def swap(x, count):
    return lax.ppermute(x, AXES, [(i, i ^ 1) for i in range(count)])


def near_or_far(x, count):
    pairs = [(i, i + 1 if i % 2 == 0 else (i + REACH - 1) % count) for i in range(count)]
    return lax.ppermute(x, AXES, pairs)


def attend_kernel(groups, sizes, docs, lens_ref, q_ref, *refs):
    count = len([p for g in groups for p in g])
    piece_refs = refs[:count]
    out_ref, qhl, vt, acc, top = refs[count:]
    tok, heads = sizes
    rows = tok * heads
    dim = q_ref.shape[1]
    tile = 256
    ones_rows = vt.shape[0] - dim
    me = lax.axis_index("outer") * lax.axis_size("inner") + lax.axis_index("inner")
    odd = lax.rem(me, 2)
    q_start = me * tok

    def bounds(k, carry):
        start, first, last = carry
        first = jnp.where(start <= q_start, start, first)
        last = jnp.where(start <= q_start + tok - 1, start, last)
        return start + lens_ref[k], first, last

    zero = jnp.int32(0)
    _, lo_first, lo_last = lax.fori_loop(0, docs, bounds, (zero, zero, zero))

    q = q_ref[...].astype(jnp.float32) * (dim ** -0.5 / math.log(2.0))
    high = q.astype(jnp.bfloat16)
    qhl[:, :dim] = high
    qhl[:, dim:] = (q - high.astype(jnp.float32)).astype(jnp.bfloat16)
    acc[...] = jnp.zeros_like(acc)
    top[...] = jnp.full(top.shape, NEG, jnp.float32)

    index = 0
    for group in groups:
        kvs = piece_refs[index:index + len(group)]
        index += len(group)
        keys = len(group) * tok
        begins = [(me - (even + (at_odd - even) * odd)) * tok for even, at_odd in group]
        live = [(b >= 0) & (b + tok - 1 >= lo_first) & (b <= q_start) for b in begins]
        full = [(b >= lo_last) & (b + tok - 1 <= q_start) for b in begins]
        any_live = functools.reduce(jnp.logical_or, live)
        all_full = functools.reduce(jnp.logical_and, full)

        def process(masked, kvs=kvs, begins=begins, keys=keys):
            k = jnp.concatenate([kv[0] for kv in kvs], axis=0)
            k2 = jnp.concatenate([k, k], axis=1)
            for n, kv in enumerate(kvs):
                vt[:dim, n * tok:(n + 1) * tok] = kv[1].T
            vt[dim:, :keys] = jnp.ones((ones_rows, keys), jnp.bfloat16)
            v = vt[:, :keys]
            for at in range(0, rows, tile):
                cols = pl.ds(at, tile)
                s = lax.dot_general(
                    k2, qhl[cols, :], (((1,), (1,)), ((), ())),
                    preferred_element_type=jnp.float32,
                )
                if masked:
                    q_pos = q_start + (at + lax.broadcasted_iota(jnp.int32, (1, tile), 1)) // heads

                    def low(i, carry, q_pos=q_pos):
                        start, lo = carry
                        return start + lens_ref[i], jnp.where(start <= q_pos, start, lo)

                    _, lo = lax.fori_loop(0, docs, low, (zero, jnp.zeros_like(q_pos)))
                    k_pos = jnp.concatenate(
                        [b + lax.broadcasted_iota(jnp.int32, (tok, 1), 0) for b in begins], axis=0
                    )
                    s = jnp.where((k_pos >= lo) & (k_pos <= q_pos), s, NEG)
                old = top[:, cols]
                new = jnp.maximum(old, jnp.max(s, axis=0, keepdims=True))
                p = jnp.exp2(s - new).astype(jnp.bfloat16)
                o = lax.dot_general(
                    v, p, (((1,), (0,)), ((), ())), preferred_element_type=jnp.float32
                )
                acc[:, cols] = acc[:, cols] * jnp.exp2(old - new) + o
                top[:, cols] = new

        pl.when(all_full)(functools.partial(process, False))
        pl.when(any_live & jnp.logical_not(all_full))(functools.partial(process, True))

    for at in range(0, rows, dim):
        cols = pl.ds(at, dim)
        o = acc[:dim, cols] * (1.0 / acc[dim:dim + 1, cols])
        out_ref[cols, :] = o.T.astype(jnp.bfloat16)


def attend(queries, lens, groups, pieces):
    tok, heads, dim = queries.shape
    rows = tok * heads
    widest = max(len(g) for g in groups) * tok
    vmem = pl.BlockSpec(memory_space=pltpu.VMEM)
    kernel = functools.partial(attend_kernel, groups, (tok, heads), lens.shape[0])
    out = pl.pallas_call(
        kernel,
        out_shape=jax.ShapeDtypeStruct((rows, dim), jnp.bfloat16),
        in_specs=[pl.BlockSpec(memory_space=pltpu.SMEM)] + [vmem] * (1 + len(pieces)),
        out_specs=vmem,
        scratch_shapes=[
            pltpu.VMEM((rows, 2 * dim), jnp.bfloat16),
            pltpu.VMEM((dim + 16, widest), jnp.bfloat16),
            pltpu.VMEM((dim + 16, rows), jnp.float32),
            pltpu.VMEM((1, rows), jnp.float32),
        ],
        compiler_params=pltpu.CompilerParams(vmem_limit_bytes=24 * 1024 * 1024),
        name="attend",
    )(lens, queries.reshape(rows, dim), *pieces)
    return out.reshape(tok, heads, dim)


def body(count, queries, key_vectors, value_vectors, doc_lengths):
    half = REACH // 2
    own = jnp.stack([key_vectors, value_vectors])
    a = {0: own}
    b = {}
    for k in range(1, half // 2):
        a[k] = rotate(own, count, 2 * k)
    a[half // 2] = rotate(own, count, half)
    b[0] = near_or_far(own, count)
    for k in range(1, half // 2 + 1):
        b[k] = swap(a[k], count)
    for k in range(1, half // 2):
        a[half // 2 + k] = rotate(a[k], count, half)
    for k in range(1, half // 2):
        b[half // 2 + k] = rotate(b[k], count, half)

    def at(kind, k):
        if kind == "a":
            return (2 * k, 2 * k)
        if k == 0:
            return (REACH - 1, 1)
        return (2 * k - 1, 2 * k + 1)

    order = [("a", k) for k in range(half)] + [("b", k) for k in range(half)]
    groups = [order[n:n + 4] for n in range(0, len(order), 4)]
    pieces = [(a if kind == "a" else b)[k] for kind, k in order]
    distances = [[at(kind, k) for kind, k in g] for g in groups]
    return attend(queries, doc_lengths, distances, pieces)


def solution(mesh):
    count = mesh.shape["outer"] * mesh.shape["inner"]
    row = P(AXES, None)
    return jax.shard_map(
        functools.partial(body, count), mesh=mesh,
        in_specs=(P(AXES, None, None), row, row, P()),
        out_specs=P(AXES, None, None), check_vma=False,
    )
```

```python
import functools
import math

import jax
import jax.numpy as jnp
from jax import lax
from jax.experimental import pallas as pl
from jax.experimental.pallas import tpu as pltpu
from jax.sharding import PartitionSpec as P

REACH = 16
AXES = ("outer", "inner")
NEG = -1e30
MIB = 1024 * 1024
SMEM = pl.BlockSpec(memory_space=pltpu.SMEM)
VMEM = pl.BlockSpec(memory_space=pltpu.VMEM)


def permute(x, target, count):
    return lax.ppermute(x, AXES, [(i, target(i) % count) for i in range(count)])


def prepare_kernel(tok, heads, q_ref, qt_ref, wide):
    dim = q_ref.shape[1]
    wide[...] = q_ref[...].astype(jnp.float32) * (dim ** -0.5 / math.log(2.0))
    for h in range(heads):
        x = wide[pl.ds(h, tok, stride=heads), :].T
        high = x.astype(jnp.bfloat16)
        cols = slice(h * tok, (h + 1) * tok)
        qt_ref[:dim, cols] = high
        qt_ref[dim:, cols] = (x - high.astype(jnp.float32)).astype(jnp.bfloat16)


def prepare(queries):
    tok, heads, dim = queries.shape
    rows = tok * heads
    return pl.pallas_call(
        functools.partial(prepare_kernel, tok, heads),
        out_shape=jax.ShapeDtypeStruct((2 * dim, rows), jnp.bfloat16),
        in_specs=[VMEM],
        out_specs=VMEM,
        scratch_shapes=[pltpu.VMEM((rows, dim), jnp.float32)],
        compiler_params=pltpu.CompilerParams(vmem_limit_bytes=8 * MIB),
        cost_estimate=pl.CostEstimate(
            flops=600_000_000, bytes_accessed=rows * dim * 6, transcendentals=0
        ),
        name="prepare",
    )(queries.reshape(rows, dim))


def step_kernel(distances, shape, docs, first, last, lens_ref, qt_ref, *refs):
    tok, heads, dim = shape
    rows, keys = tok * heads, len(distances) * tok
    tile = min(4, heads) * tok
    kv_refs, refs = refs[:len(distances)], refs[len(distances):]
    if not first:
        acc_in, top_in, *refs = refs
    if last:
        out_ref, wide, vt, bias = refs
    else:
        acc_out, top_out, vt, bias = refs
    me = lax.axis_index("outer") * lax.axis_size("inner") + lax.axis_index("inner")
    odd = lax.rem(me, 2)
    q_start = me * tok
    begins = [(me - (even + (at_odd - even) * odd)) * tok for even, at_odd in distances]

    def first_start(i, carry):
        start, lo = carry
        return start + lens_ref[i], jnp.where(start <= q_start, start, lo)

    def starts(q_pos):
        def step(i, carry):
            start, lo = carry
            return start + lens_ref[i], jnp.where(start <= q_pos, start, lo)
        return lax.fori_loop(0, docs, step, (jnp.int32(0), jnp.zeros_like(q_pos)))[1]

    lo_first = lax.fori_loop(0, docs, first_start, (jnp.int32(0), jnp.int32(0)))[1]
    live = functools.reduce(
        jnp.logical_or,
        [(b >= 0) & (b + tok > lo_first) & (b <= q_start) for b in begins],
    )

    def emit(h, o):
        wide[pl.ds(h, tok, stride=heads), :] = (o[:dim] * (1.0 / o[dim:dim + 1])).T

    def process():
        k = jnp.concatenate([kv[0] for kv in kv_refs], axis=0)
        k2 = jnp.concatenate([k, k], axis=1)
        for n, kv in enumerate(kv_refs):
            vt[:dim, n * tok:(n + 1) * tok] = kv[1].T
        vt[dim:, :] = jnp.ones((vt.shape[0] - dim, keys), jnp.bfloat16)
        q_pos = q_start + lax.broadcasted_iota(jnp.int32, (1, tok), 1)
        lo = starts(q_pos)
        for n, b in enumerate(begins):
            k_pos = b + lax.broadcasted_iota(jnp.int32, (tok, 1), 0)
            seen = (k_pos >= lo) & (k_pos <= q_pos)
            bias[n * tok:(n + 1) * tok, :] = jnp.where(seen, 0.0, NEG)

        def score(at):
            return lax.dot_general(
                k2, qt_ref[:, at:at + tile], (((1,), (0,)), ((), ())),
                preferred_element_type=jnp.float32,
            )

        def soften(at, s):
            s = s + jnp.concatenate([bias[...]] * (tile // tok), axis=1)
            new = jnp.max(s, axis=0, keepdims=True)
            scale = None
            if not first:
                old = top_in[:, at:at + tile]
                new = jnp.maximum(old, new)
                scale = jnp.exp2(old - new)
            if not last:
                top_out[:, at:at + tile] = new
            return at, jnp.exp2(s - new).astype(jnp.bfloat16), scale

        def fold(at, p, scale):
            o = lax.dot_general(
                vt[...], p, (((1,), (0,)), ((), ())), preferred_element_type=jnp.float32
            )
            if not first:
                o = acc_in[:, at:at + tile] * scale + o
            if last:
                for n in range(tile // tok):
                    emit(at // tok + n, o[:, n * tok:(n + 1) * tok])
            else:
                acc_out[:, at:at + tile] = o

        s, held = score(0), None
        for at in range(0, rows, tile):
            ahead = score(at + tile) if at + tile < rows else None
            now = soften(at, s)
            if held is not None:
                fold(*held)
            held, s = now, ahead
        fold(*held)

    if first:
        process()
    else:
        pl.when(live)(process)

        @pl.when(jnp.logical_not(live))
        def _():
            if last:
                for h in range(heads):
                    emit(h, acc_in[:, h * tok:(h + 1) * tok])
            else:
                acc_out[...] = acc_in[...]
                top_out[...] = top_in[...]

    if last:
        out_ref[...] = wide[...].astype(jnp.bfloat16)


def attend(qt, lens, shape, blocks, state, last, name):
    tok, heads, dim = shape
    rows = tok * heads
    first = state is None
    pieces, distances = [b[0] for b in blocks], [b[1] for b in blocks]
    keys = len(pieces) * tok
    sums = dim + 16
    scratch = [pltpu.VMEM((sums, keys), jnp.bfloat16), pltpu.VMEM((keys, tok), jnp.float32)]
    if last:
        out_shape = jax.ShapeDtypeStruct((rows, dim), jnp.bfloat16)
        out_specs = VMEM
        scratch = [pltpu.VMEM((rows, dim), jnp.float32)] + scratch
    else:
        out_shape = [
            jax.ShapeDtypeStruct((sums, rows), jnp.float32),
            jax.ShapeDtypeStruct((1, rows), jnp.float32),
        ]
        out_specs = [VMEM, VMEM]
    carried = [] if first else list(state)
    return pl.pallas_call(
        functools.partial(step_kernel, distances, shape, lens.shape[0], first, last),
        out_shape=out_shape,
        in_specs=[SMEM] + [VMEM] * (1 + len(pieces) + len(carried)),
        out_specs=out_specs,
        scratch_shapes=scratch,
        compiler_params=pltpu.CompilerParams(vmem_limit_bytes=16 * MIB),
        cost_estimate=pl.CostEstimate(
            flops=4 * rows * keys * dim, bytes_accessed=rows * keys, transcendentals=rows * keys
        ),
        name=name,
    )(lens, qt, *pieces, *carried)


def body(count, queries, key_vectors, value_vectors, doc_lengths):
    half = REACH // 2
    shape = queries.shape
    own = jnp.stack([key_vectors, value_vectors])

    def along(k):
        return lambda i: i + 2 * k

    def mate(i):
        return i ^ 1

    def group(i):
        return i + half

    def group_mate(i):
        return (i ^ 1) + half

    def edge(i):
        return i + 1 if i % 2 == 0 else i + REACH - 1

    def send(x, target):
        return permute(x, target, count)

    def send_all(xs, target):
        both = send(jnp.concatenate(xs, axis=0), target)
        return [both[2 * n:2 * n + 2] for n in range(len(xs))]

    a, b = {0: own}, {}
    a[3] = send(own, along(3))
    a[2] = send(own, along(2))
    a[1] = send(own, along(1))
    a[4] = send(own, group)
    b[0] = send(own, edge)
    b[4], b[1] = send_all([a[4], a[1]], mate)
    b[2] = send(a[2], mate)
    a[5], a[6] = send_all([a[1], a[2]], group)
    b[3] = send(a[3], mate)
    a[7] = send(a[3], group)
    b[7] = send(a[3], group_mate)
    b[5], b[6] = send_all([b[1], b[2]], group)

    def block(kind, k):
        if kind == "a":
            return a[k], (2 * k, 2 * k)
        if k == 0:
            return b[0], (REACH - 1, 1)
        return b[k], (2 * k - 1, 2 * k + 1)

    plan = [
        [("a", 0), ("a", 4), ("b", 0)],
        [("a", 1), ("a", 2), ("a", 3)],
        [("b", 4), ("b", 1), ("b", 2), ("a", 5), ("a", 6)],
        [("b", 3), ("a", 7), ("b", 7), ("b", 5), ("b", 6)],
    ]
    qt = prepare(queries)
    state = None
    for n, names in enumerate(plan):
        blocks = [block(*name) for name in names]
        state = attend(qt, doc_lengths, shape, blocks, state, n == len(plan) - 1, f"attend{n}")
    return state.reshape(shape)


def solution(mesh):
    count = mesh.shape["outer"] * mesh.shape["inner"]
    row = P(AXES, None)
    return jax.shard_map(
        functools.partial(body, count), mesh=mesh,
        in_specs=(P(AXES, None, None), row, row, P()),
        out_specs=P(AXES, None, None), check_vma=False,
    )
```

```python
import functools
import math

import jax
import jax.numpy as jnp
from jax import lax
from jax.experimental import pallas as pl
from jax.experimental.pallas import tpu as pltpu
from jax.sharding import PartitionSpec as P

REACH = 16
AXES = ("outer", "inner")
NEG = -1e30
SAFE = 2.0 ** 120
MIB = 1024 * 1024
SMEM = pl.BlockSpec(memory_space=pltpu.SMEM)
VMEM = pl.BlockSpec(memory_space=pltpu.VMEM)
ANY = pl.BlockSpec(memory_space=pl.ANY)


def position(tok):
    me = lax.axis_index("outer") * lax.axis_size("inner") + lax.axis_index("inner")
    return me, me * tok


def block_begins(me, tok, distances):
    odd = lax.rem(me, 2)
    return [(me - (even + (at_odd - even) * odd)) * tok for even, at_odd in distances]


def document_start(lens_ref, docs, q_pos):
    def step(i, carry):
        start, lo = carry
        return start + lens_ref[i], jnp.where(start <= q_pos, start, lo)

    return lax.fori_loop(0, docs, step, (jnp.int32(0), jnp.zeros_like(q_pos)))[1]


def any_live(begins, tok, q_start, lo_first):
    return functools.reduce(
        jnp.logical_or,
        [(b >= 0) & (b + tok > lo_first) & (b <= q_start) for b in begins],
    )


def mask_of(begin, tok, lo, q_pos):
    k_pos = begin + lax.broadcasted_iota(jnp.int32, (tok, 1), 0)
    return jnp.where((k_pos >= lo) & (k_pos <= q_pos), 0.0, NEG)


def mm(a, b):
    return lax.dot_general(
        a, b, (((1,), (0,)), ((), ())), preferred_element_type=jnp.float32
    )


def twice(k):
    return jnp.concatenate([k, k], axis=1)


def open_kernel(shape, docs, lens_ref, q_ref, kv_ref, qt_ref, acc_ref, top_ref, wide):
    tok, heads, dim = shape
    _, q_start = position(tok)
    q_pos = q_start + lax.broadcasted_iota(jnp.int32, (1, tok), 1)
    bias = mask_of(q_start, tok, document_start(lens_ref, docs, q_pos), q_pos)
    k2 = twice(kv_ref[0])
    ones = jnp.ones((acc_ref.shape[0] - dim, tok), jnp.bfloat16)
    vt = jnp.concatenate([kv_ref[1].T, ones], axis=0)
    wide[...] = q_ref[...].astype(jnp.float32) * (dim ** -0.5 / math.log(2.0))
    span = 2 if heads % 2 == 0 else 1
    tile = span * tok

    def ready(at):
        for h in range(at // tok, at // tok + span):
            x = wide[pl.ds(h, tok, stride=heads), :].T
            high = x.astype(jnp.bfloat16)
            cols = slice(h * tok, (h + 1) * tok)
            qt_ref[:dim, cols] = high
            qt_ref[dim:, cols] = (x - high.astype(jnp.float32)).astype(jnp.bfloat16)
        return mm(k2, qt_ref[:, at:at + tile])

    def soften(at, s):
        s = s + jnp.concatenate([bias] * span, axis=1)
        top = jnp.max(s, axis=0, keepdims=True)
        top_ref[:, at:at + tile] = top
        return at, jnp.exp2(s - top).astype(jnp.bfloat16)

    def fold(at, p):
        acc_ref[:, at:at + tile] = mm(vt, p)

    s, held = ready(0), None
    for at in range(0, tok * heads, tile):
        ahead = ready(at + tile) if at + tile < tok * heads else None
        now = soften(at, s)
        if held is not None:
            fold(*held)
        held, s = now, ahead
    fold(*held)


def accumulate(shape, kv_refs, begins, lo, q_pos, qt_ref, top_ref, vt, bias, fold):
    tok, heads, dim = shape
    keys = len(kv_refs) * tok
    k2 = twice(jnp.concatenate([kv[0] for kv in kv_refs], axis=0))
    for n, kv in enumerate(kv_refs):
        vt[:dim, n * tok:(n + 1) * tok] = kv[1].T
    vt[dim:, :keys] = jnp.ones((vt.shape[0] - dim, keys), jnp.bfloat16)
    for n, b in enumerate(begins):
        bias[n * tok:(n + 1) * tok, :] = mask_of(b, tok, lo, q_pos)
    span = 2 if heads % 2 == 0 else 1
    tile = span * tok

    def score(at):
        return mm(k2, qt_ref[:, at:at + tile])

    def soften(at, s):
        mask = jnp.concatenate([bias[:keys, :]] * span, axis=1)
        return at, jnp.exp2((s - top_ref[:, at:at + tile]) + mask).astype(jnp.bfloat16)

    s, held = score(0), None
    for at in range(0, tok * heads, tile):
        ahead = score(at + tile) if at + tile < tok * heads else None
        now = soften(at, s)
        if held is not None:
            fold(held[0], tile, mm(vt[:, :keys], held[1]))
        held, s = now, ahead
    fold(held[0], tile, mm(vt[:, :keys], held[1]))


def emit(shape, wide, at, width, o):
    tok, heads, dim = shape
    for n in range(width // tok):
        part = o[:, n * tok:(n + 1) * tok]
        scaled = part[:dim] * (1.0 / part[dim:dim + 1])
        wide[pl.ds(at // tok + n, tok, stride=heads), :] = scaled.T


def put(wide, narrow, out_ref, sem):
    narrow[...] = wide[...].astype(jnp.bfloat16)
    copy = pltpu.make_async_copy(narrow, out_ref, sem)
    copy.start()
    copy.wait()


def middle_kernel(
    shape, docs, distances, rest, closing, lens_ref, qt_ref, top_ref, acc_in, *refs
):
    tok, heads, dim = shape
    kv_refs, refs = refs[:len(distances)], refs[len(distances):]
    if closing:
        acc_ref, out_ref, vt, bias, wide, narrow, sem = refs
    else:
        acc_ref, vt, bias = refs
    me, q_start = position(tok)
    q_pos = q_start + lax.broadcasted_iota(jnp.int32, (1, tok), 1)
    begins = block_begins(me, tok, distances)
    lo_first = document_start(lens_ref, docs, q_start)
    live = any_live(begins, tok, q_start, lo_first)

    def fold(at, width, o):
        acc_ref[:, at:at + width] = acc_in[:, at:at + width] + o

    @pl.when(live)
    def _():
        lo = document_start(lens_ref, docs, q_pos)
        accumulate(
            shape, kv_refs, begins, lo, q_pos, qt_ref, top_ref, vt, bias, fold
        )

    if closing:
        later = any_live(block_begins(me, tok, rest), tok, q_start, lo_first)

        @pl.when(jnp.logical_not(later))
        def _():
            for at in range(0, tok * heads, tok):
                emit(shape, wide, at, tok, acc_ref[:, at:at + tok])
            put(wide, narrow, out_ref, sem)


def last_kernel(
    shape, docs, distances, everything, lens_ref, qt_ref, top_ref, acc_in, old_ref, *refs
):
    tok, heads, dim = shape
    all_refs, refs = refs[:len(everything)], refs[len(everything):]
    out_ref, vt, bias, wide, narrow, total, sem = refs
    kv_refs = all_refs[len(everything) - len(distances):]
    me, q_start = position(tok)
    q_pos = q_start + lax.broadcasted_iota(jnp.int32, (1, tok), 1)
    begins = block_begins(me, tok, distances)
    lo_first = document_start(lens_ref, docs, q_start)
    live = any_live(begins, tok, q_start, lo_first)
    total[...] = acc_in[dim:dim + 1, :]

    @pl.when(live)
    def _():
        def fold(at, width, o):
            o = acc_in[:, at:at + width] + o
            total[:, at:at + width] = o[dim:dim + 1]
            emit(shape, wide, at, width, o)

        lo = document_start(lens_ref, docs, q_pos)
        accumulate(
            shape, kv_refs, begins, lo, q_pos, qt_ref, top_ref, vt, bias, fold
        )
        put(wide, narrow, out_ref, sem)

    fine = jnp.min(jnp.where(total[...] < SAFE, 1.0, 0.0)) > 0.5

    @pl.when(jnp.logical_not(fine))
    def _():
        every = block_begins(me, tok, everything)
        lo = document_start(lens_ref, docs, q_pos)

        def head(h, carry):
            cols = pl.ds(pl.multiple_of(h * tok, tok), tok)
            top = jnp.full((1, tok), NEG, jnp.float32)
            acc = jnp.zeros((vt.shape[0], tok), jnp.float32)
            ones = jnp.ones((vt.shape[0] - dim, tok), jnp.bfloat16)
            for kv, b in zip(all_refs, every):
                s = mm(twice(kv[0]), qt_ref[:, cols]) + mask_of(b, tok, lo, q_pos)
                new = jnp.maximum(top, jnp.max(s, axis=0, keepdims=True))
                p = jnp.exp2(s - new).astype(jnp.bfloat16)
                values = jnp.concatenate([kv[1].T, ones], axis=0)
                acc = acc * jnp.exp2(top - new) + mm(values, p)
                top = new
            scaled = acc[:dim] * (1.0 / acc[dim:dim + 1])
            wide[pl.ds(h, tok, stride=heads), :] = scaled.T
            return carry

        lax.fori_loop(0, heads, head, 0)
        put(wide, narrow, out_ref, sem)


def params(mib=16):
    return pltpu.CompilerParams(vmem_limit_bytes=mib * MIB)


def cost(shape, blocks):
    tok, heads, dim = shape
    pairs = tok * heads * tok * blocks
    return pl.CostEstimate(
        flops=8 * pairs * dim, bytes_accessed=6 * tok * heads * dim, transcendentals=pairs
    )


def opened(queries, lens, own):
    shape = tok, heads, dim = queries.shape
    rows = tok * heads
    return pl.pallas_call(
        functools.partial(open_kernel, shape, lens.shape[0]),
        out_shape=[
            jax.ShapeDtypeStruct((2 * dim, rows), jnp.bfloat16),
            jax.ShapeDtypeStruct((dim + 16, rows), jnp.float32),
            jax.ShapeDtypeStruct((1, rows), jnp.float32),
        ],
        in_specs=[SMEM, VMEM, VMEM],
        out_specs=[VMEM] * 3,
        scratch_shapes=[pltpu.VMEM((rows, dim), jnp.float32)],
        compiler_params=params(8),
        cost_estimate=cost(shape, 3),
        name="open",
    )(lens, queries.reshape(rows, dim), own)


def middle(shape, lens, qt, top, acc, blocks, rest, name):
    tok, heads, dim = shape
    rows = tok * heads
    keys = len(blocks) * tok
    closing = rest is not None
    pieces, distances = [b[0] for b in blocks], [b[1] for b in blocks]
    out_shape = [jax.ShapeDtypeStruct((dim + 16, rows), jnp.float32)]
    scratch = [pltpu.VMEM((dim + 16, keys), jnp.bfloat16), pltpu.VMEM((keys, tok), jnp.float32)]
    if closing:
        out_shape.append(jax.ShapeDtypeStruct((rows, dim), jnp.bfloat16))
        scratch += [
            pltpu.VMEM((rows, dim), jnp.float32),
            pltpu.VMEM((rows, dim), jnp.bfloat16),
            pltpu.SemaphoreType.DMA,
        ]
    return pl.pallas_call(
        functools.partial(middle_kernel, shape, lens.shape[0], distances, rest, closing),
        out_shape=out_shape,
        in_specs=[SMEM] + [VMEM] * (3 + len(pieces)),
        out_specs=[VMEM, ANY][:len(out_shape)],
        scratch_shapes=scratch,
        input_output_aliases={3: 0},
        compiler_params=params(),
        cost_estimate=cost(shape, len(blocks)),
        name=name,
    )(lens, qt, top, acc, *pieces)


def last(shape, lens, qt, top, acc, out, earlier, blocks):
    tok, heads, dim = shape
    rows = tok * heads
    keys = len(blocks) * tok
    pieces = [b[0] for b in earlier + blocks]
    everything = [b[1] for b in earlier + blocks]
    distances = [b[1] for b in blocks]
    return pl.pallas_call(
        functools.partial(last_kernel, shape, lens.shape[0], distances, everything),
        out_shape=jax.ShapeDtypeStruct((rows, dim), jnp.bfloat16),
        in_specs=[SMEM] + [VMEM] * 3 + [ANY] + [VMEM] * len(pieces),
        out_specs=ANY,
        scratch_shapes=[
            pltpu.VMEM((dim + 16, keys), jnp.bfloat16),
            pltpu.VMEM((keys, tok), jnp.float32),
            pltpu.VMEM((rows, dim), jnp.float32),
            pltpu.VMEM((rows, dim), jnp.bfloat16),
            pltpu.VMEM((1, rows), jnp.float32),
            pltpu.SemaphoreType.DMA,
        ],
        input_output_aliases={4: 0},
        compiler_params=params(),
        cost_estimate=cost(shape, len(blocks)),
        name="last",
    )(lens, qt, top, acc, out, *pieces)


def body(count, queries, key_vectors, value_vectors, doc_lengths):
    half = REACH // 2
    shape = queries.shape
    own = jnp.stack([key_vectors, value_vectors])
    moves = {
        "z1": lambda i: i + 2,
        "z2": lambda i: i + 4,
        "z3": lambda i: i + 6,
        "x": lambda i: i ^ 1,
        "y": lambda i: i + half,
        "xy": lambda i: (i ^ 1) + half,
        "r": lambda i: i + 1 if i % 2 == 0 else i + REACH - 1,
    }

    def move(x, name):
        return lax.ppermute(x, AXES, [(i, moves[name](i) % count) for i in range(count)])

    def move_all(xs, name):
        joined = move(jnp.concatenate(xs, axis=0), name)
        return [joined[2 * n:2 * n + 2] for n in range(len(xs))]

    a, b = {0: own}, {}
    a[3] = move(own, "z3")
    a[2] = move(own, "z2")
    a[1] = move(own, "z1")
    a[4] = move(own, "y")
    b[0] = move(own, "r")
    b[4], b[1] = move_all([a[4], a[1]], "x")
    b[2] = move(a[2], "x")
    a[5], a[6] = move_all([a[1], a[2]], "y")
    b[3] = move(a[3], "x")
    a[7] = move(a[3], "y")
    b[7] = move(a[3], "xy")
    b[5], b[6] = move_all([b[1], b[2]], "y")

    def block(kind, k):
        if kind == "a":
            return a[k], (2 * k, 2 * k)
        if k == 0:
            return b[0], (REACH - 1, 1)
        return b[k], (2 * k - 1, 2 * k + 1)

    plan = [[block(*name) for name in group] for group in (
        [("a", 4), ("b", 0), ("a", 1), ("a", 2), ("a", 3), ("b", 4), ("b", 1), ("b", 2), ("b", 3)],
        [("a", 5), ("a", 6), ("a", 7), ("b", 7), ("b", 5), ("b", 6)],
    )]
    far = [d for _, d in plan[-1]]
    qt, acc, top = opened(queries, doc_lengths, own)
    for n, group in enumerate(plan[:-1]):
        closing = n == len(plan) - 2
        acc, *out = middle(
            shape, doc_lengths, qt, top, acc, group, far if closing else None, f"middle{n}"
        )
    earlier = [block("a", 0)] + [one for group in plan[:-1] for one in group]
    done = last(shape, doc_lengths, qt, top, acc, out[0], earlier, plan[-1])
    return done.reshape(shape)


def solution(mesh):
    count = mesh.shape["outer"] * mesh.shape["inner"]
    row = P(AXES, None)
    return jax.shard_map(
        functools.partial(body, count), mesh=mesh,
        in_specs=(P(AXES, None, None), row, row, P()),
        out_specs=P(AXES, None, None), check_vma=False,
    )
```
